128 devices in a mesh: grp: 4 (over x), seq: 32 (over y, z, core).
Axes of the slice: x: 4, y: 4, z: 4, core: 2. Of those that a mesh axis runs over, the one named last changes fastest.
Arguments:
- tokens: bfloat16 [8192, 8192], P(None, 'seq'), may hold values from -16 to 16
- proj_weight: bfloat16 [8192, 5120], P('seq', 'grp'), may hold values from -0.0625 to 0.0625
- proj_bias: bfloat16 [5120], P('grp'), may hold values from -3 to 3
- out_weight: bfloat16 [4096, 8192], P('grp'), may hold values from -0.125 to 0.125
- doc_ids: int32 [8192], P('seq'), may hold values from 0 to 2, never falling along the last dimension, each value on 1 to 4352 neighbouring positions
Outputs:
- mixed: bfloat16 [8192, 8192], P('seq', 'grp')
The draws below stay inside these ranges and needn't reach their ends.
Inputs may be any that keep to these rules, and one draw needn't show every extreme that they name: `doc_ids`: numbers never fall along the sequence; every document has 1 to 4352 tokens, one exactly that many; every number up to 2 is used.
All inputs are finite; a program needn't handle non-finite values.
Results may differ from the reference program's by a relative error of at most 0.012.
Values may be sent and summed in bfloat16 or wider, within the bound.
No kernel may reach another device: no remote copies, remote signals or barrier semaphores. Data moves between devices by JAX's collectives and lax.ppermute only.
A program may use at most 256 MiB of HBM per device.

```python
import math
import jax
import jax.numpy as jnp
import numpy as np
from jax import lax

D = 8192
Q_HEADS = 32
KV_HEADS = 4
HEAD_DIM = 128
TOK_DEV = 256
SPAN = 17
GQA = 8
TOKENS = 8192
DOCS = 3


def draw_tokens(key, part):
    normals = jax.random.normal(jax.random.fold_in(key, 11), (TOKENS, D), jnp.float32)
    block_offsets = jax.random.normal(jax.random.fold_in(key, 19), (TOKENS // TOK_DEV, D), jnp.float32)
    offset_rows = jnp.repeat(block_offsets, TOK_DEV, axis=0)
    result = jnp.clip(normals + 1.5 * offset_rows, -8.0, 8.0)
    return result.astype(jnp.bfloat16)


def with_spikes(drawn, own_key, source, target, shards_of, factor):
    owner, partner = [(jnp.arange(drawn.shape[position]) // (drawn.shape[position] // shards_of)).reshape([-1 if axis == position else 1 for axis in range(drawn.ndim)]) for position in (source, target)]
    chosen = jax.random.permutation(own_key, shards_of)[partner]
    strong = (owner == chosen) | (owner == (partner + shards_of // 2) % shards_of)
    return jnp.where(strong, factor * drawn, drawn)


def block_scale(own_key, extent, shards, low, largest):
    def one(axis_at, parts):
        draws = jax.random.uniform(jax.random.fold_in(jax.random.fold_in(own_key, 6), axis_at), (parts,), jnp.float32, low / len(shards), largest / len(shards))
        return jnp.repeat(jnp.exp(draws), extent[axis_at] // parts).reshape((-1,) + (1,) * (len(extent) - axis_at - 1))

    level = one(*shards[0])
    for cut in shards[1:]:
        level = level * one(*cut)
    return level


def split_up(number_of, total, limit, slope):
    weights = [(1 << 20) // math.isqrt(standing ** slope) + 1 for standing in range(2, number_of + 1)]
    spare, holding = total - limit - (number_of - 1), [1] * (number_of - 1)
    while spare > 0:
        movable = [i for i in range(number_of - 1) if holding[i] < limit]
        pool, remaining = sum([weights[i] for i in movable]), spare
        for i in movable:
            more = min(limit - holding[i], max(1, remaining * weights[i] // pool), spare)
            holding[i] = holding[i] + more
            spare = spare - more
    return np.array([limit] + holding)


def ragged_sizes(key, amount, total, limit, slope):
    if amount == 2:
        one = jax.random.randint(key, (), max(1, total - limit), min(limit, total - 1) + 1)
        return jnp.stack([one, total - one])
    sizes = jnp.asarray(split_up(amount, total, limit, slope), jnp.int32)
    twos = (amount - 1) // 2
    donor, sink = sizes[1:1 + 2 * twos:2], sizes[2:2 + 2 * twos:2]
    room = jnp.minimum(donor - 1, limit - sink)
    shifted = jax.random.randint(jax.random.fold_in(key, 1), (twos,), 0, 1 << 20) % (room + 1)
    sizes = sizes.at[1:1 + 2 * twos:2].set(donor - shifted).at[2:2 + 2 * twos:2].set(sink + shifted)
    return sizes[jax.random.permutation(jax.random.fold_in(key, 2), amount)]


def normal_values(rng, shape, scale, reach, split=(), held_as=jnp.bfloat16):
    drawn = jax.random.normal(rng, shape, jnp.float32) * scale
    if len(split) > 0:
        drawn = block_scale(rng, shape, split, -0.22, 0.18) * drawn
    return jnp.clip(drawn, min=-reach, max=reach).astype(held_as)


def bell_draw_with(own_key, extent, deviation, limit, split, heavy, kind=jnp.bfloat16):
    array = deviation * jax.random.normal(own_key, extent, jnp.float32)
    if split:
        array = array * block_scale(own_key, extent, split, -0.22, 0.18)
    return jnp.clip(with_spikes(array, jax.random.fold_in(own_key, 3), *heavy), -limit, limit).astype(kind)


def setup_inputs(seed: int = 0) -> dict:
    splits = jax.random.split(jax.random.key(seed), 6)
    tokens = draw_tokens(jax.random.fold_in(splits[5], 71), 0)
    proj_weight = normal_values(splits[1], (D, KV_HEADS * (GQA + 2) * HEAD_DIM), D ** -0.5, 0.0625, ((0, 32), (1, 4)))
    proj_bias = normal_values(splits[2], (KV_HEADS * (GQA + 2) * HEAD_DIM,), 0.5, 3.0, ((0, 4),))
    out_weight = bell_draw_with(splits[3], (Q_HEADS * HEAD_DIM, D), (Q_HEADS * HEAD_DIM) ** -0.5, 0.125, ((0, 4),), (0, 1, 4, 2.0))
    doc_ids = jnp.searchsorted(jnp.cumsum(ragged_sizes(splits[4], DOCS, TOKENS, SPAN * TOK_DEV, 1)), jnp.arange(TOKENS), side="right").astype(jnp.int32)
    return dict(tokens=tokens, proj_weight=proj_weight, proj_bias=proj_bias, out_weight=out_weight, doc_ids=doc_ids)


theta_base = 1000000.0


def rotate(inputs, positions, head_dim):
    half_dim = head_dim // 2
    inverse_freq = theta_base ** (-(jnp.arange(half_dim, dtype=jnp.float32) * 2.0) / head_dim)
    angles = positions.astype(jnp.float32)[:, None] * inverse_freq[None, :]
    cosine = jnp.concatenate([jnp.cos(angles), jnp.cos(angles)], axis=1)
    sine_table = jnp.concatenate([jnp.sin(angles), jnp.sin(angles)], axis=1)
    low_half = inputs[..., :half_dim]
    high_half = inputs[..., half_dim:]
    turned = jnp.concatenate([-high_half, low_half], axis=-1)
    return inputs * cosine[:, None, :] + turned * sine_table[:, None, :]


def reference(tokens, proj_weight, proj_bias, out_weight, doc_ids):
    projected = jnp.dot(tokens, proj_weight, preferred_element_type=jnp.float32) + proj_bias.astype(jnp.float32)[None, :]
    projected = projected.reshape(TOKENS, KV_HEADS, GQA + 2, HEAD_DIM)
    positions = jnp.arange(TOKENS, dtype=jnp.int32)
    queries = rotate(projected[:, :, :GQA, :].reshape(TOKENS, Q_HEADS, HEAD_DIM), positions, HEAD_DIM).astype(jnp.bfloat16)
    key_rows = rotate(projected[:, :, GQA, :], positions, HEAD_DIM).astype(jnp.bfloat16)
    value_rows = projected[:, :, GQA + 1, :].astype(jnp.bfloat16)
    allowed = (doc_ids[None, :] == doc_ids[:, None]) & (positions[None, :] <= positions[:, None])
    score_scale = HEAD_DIM ** -0.5

    def one_head(head_index):
        query_head = lax.dynamic_index_in_dim(queries, head_index, 1, keepdims=False).astype(jnp.float32)
        key_head = lax.dynamic_index_in_dim(key_rows, head_index // GQA, 1, keepdims=False).astype(jnp.float32)
        value_head = lax.dynamic_index_in_dim(value_rows, head_index // GQA, 1, keepdims=False)
        scores = jnp.dot(query_head, key_head.T, preferred_element_type=jnp.float32) * score_scale
        scores = jnp.where(allowed, scores, -jnp.inf)
        row_max = jnp.max(scores, axis=1, keepdims=True)
        weights = jnp.exp(scores - row_max)
        row_sum = jnp.sum(weights, axis=1, keepdims=True)
        summed = jnp.dot(weights.astype(jnp.bfloat16), value_head, preferred_element_type=jnp.float32)
        return (summed / row_sum).astype(jnp.bfloat16)

    head_outputs = lax.map(one_head, jnp.arange(Q_HEADS, dtype=jnp.int32))
    attended = jnp.transpose(head_outputs, (1, 0, 2)).reshape(TOKENS, Q_HEADS * HEAD_DIM)
    return jnp.dot(attended, out_weight, preferred_element_type=jnp.float32).astype(jnp.bfloat16)
```

```python
import functools
import jax
import jax.numpy as jnp
from jax import lax
from jax.experimental import pallas as pl
from jax.experimental.pallas import tpu as pltpu
from jax.sharding import Mesh, PartitionSpec as P

HEAD_DIM = 128
GQA = 8
TOK = 256
COLS = (GQA + 2) * HEAD_DIM
HALF = COLS // 2
BK = 512
theta_base = 1000000.0
NEG = -1e30
SCALE2 = HEAD_DIM ** -0.5 * 1.4426950408889634
BF = jnp.bfloat16
F32 = jnp.float32


def hop(x, axis, k, n=4):
    return lax.ppermute(x, axis, [(i, (i + k) % n) for i in range(n)])


def line_gather(x, axis):
    lo, hi, far = hop(x, axis, 1), hop(x, axis, -1), hop(x, axis, 2)
    return jnp.stack([x, lo, hi, far])


def plane_gather(a, b):
    la, lb = line_gather(a, "y"), line_gather(b, "z")
    am, ap = hop(la, "z", 1), hop(la, "z", -1)
    bm, bp = hop(lb, "y", 1), hop(lb, "y", -1)
    a0, a1 = hop(am[:2], "z", 1), hop(ap[2:], "z", -1)
    b0, b1 = hop(bm[:2], "y", 1), hop(bp[2:], "y", -1)
    return (la, am, ap, a0, a1), (lb, bm, bp, b0, b1)


def project_kernel(t0, t1, t2, t3, *refs, srcs):
    ws, out = refs[:-1], refs[-1]
    for n, (w, idx) in enumerate(zip(ws, srcs)):
        for m, s in enumerate(idx):
            lhs = jnp.concatenate([t0[s], t1[s], t2[s], t3[s]], axis=0)
            part = jnp.dot(lhs, w[m], preferred_element_type=F32)
            if n == 0 and m == 0:
                out[...] = part
            else:
                out[...] += part


def project(ts, ws, srcs):
    return pl.pallas_call(
        functools.partial(project_kernel, srcs=srcs),
        out_shape=jax.ShapeDtypeStruct((4 * 128, HALF), F32),
        name="project",
    )(*ts, *ws)


def rope(u, cos, sin):
    turned = jnp.concatenate([-u[:, HEAD_DIM // 2:], u[:, :HEAD_DIM // 2]], axis=1)
    return u * cos + turned * sin


def attend_kernel(
    info, q_in, q_got, bias, cos, sin, ids, *refs
):
    kv, (out, k_s, v_s, id_s, q_s, m_s, l_s, acc_s, sems) = refs[:20], refs[20:]
    y, z, c = info[0], info[1], info[2]
    offs = (0, -1, 1, 2)
    copies = []

    def place(src, row, dy, dz, core, which):
        by = lax.rem(y + dy + 4, 4)
        bz = lax.rem(z + dz + 4, 4)
        blk = by * 8 + bz * 2 + core
        dst = (k_s, v_s)[which]
        copies.append(pltpu.make_async_copy(
            src.at[row, pl.ds(0, TOK)], dst.at[pl.ds(pl.multiple_of(blk * TOK, TOK), TOK)], sems.at[which]))
        copies.append(pltpu.make_async_copy(
            src.at[row, pl.ds(TOK, 16)], id_s.at[which, pl.ds(pl.multiple_of(blk * 16, 16), 16)], sems.at[2 + which]))

    for side in range(2):
        core = c if side == 0 else 1 - c
        for which in range(2):
            group = kv[side * 10 + which * 5: side * 10 + which * 5 + 5]
            for arr, other, rows in zip(group, (0, -1, 1, 2, 2), (offs, offs, offs, offs[:2], offs[2:])):
                for r, o in enumerate(rows):
                    dy, dz = (o, other) if which == 0 else (other, o)
                    place(arr, r, dy, dz, core, which)
    for cp in copies:
        cp.start()
    cs, sn = cos[...], sin[...]
    for h in range(GQA):
        u = q_in[:, h * 128:(h + 1) * 128] + q_got[:, h * 128:(h + 1) * 128] + bias[:, h * 128:(h + 1) * 128].astype(F32)
        q_s[h * TOK:(h + 1) * TOK, :] = rope(u, cs, sn).astype(BF)
    m_s[...] = jnp.full_like(m_s, NEG)
    l_s[...] = jnp.zeros_like(l_s)
    acc_s[...] = jnp.zeros_like(acc_s)
    for cp in copies:
        cp.wait()
    rowsel = lax.rem(lax.broadcasted_iota(jnp.int32, (512, 128), 0), 16) == 0
    both = jnp.concatenate([id_s[0].astype(F32), id_s[1].astype(F32)], axis=1)
    sel2 = jnp.concatenate([rowsel, rowsel], axis=1)
    c1 = jnp.sum(jnp.where(sel2 & (both < 0.5), 1.0, 0.0)).astype(jnp.int32)
    c2 = jnp.sum(jnp.where(sel2 & (both < 1.5), 1.0, 0.0)).astype(jnp.int32)
    first = y * (8 * TOK) + z * (2 * TOK) + c * TOK
    mine = ids[...]
    start = jnp.where(mine == 0, 0, jnp.where(mine == 1, c1, c2))
    lo_start = jnp.where(first >= c2, c2, jnp.where(first >= c1, c1, 0))
    last = first + TOK - 1
    hi_start = jnp.where(last >= c2, c2, jnp.where(last >= c1, c1, 0))
    diag = first // BK
    lo = lo_start // BK
    full = jnp.minimum((hi_start + BK - 1) // BK, diag)
    pos = first + lax.broadcasted_iota(jnp.int32, (TOK, 1), 0)

    def block(j, masked, causal):
        base = pl.multiple_of(j * BK, BK)
        kb = k_s[pl.ds(base, BK), :]
        vb = v_s[pl.ds(base, BK), :]
        if masked or causal:
            kpos = base + lax.broadcasted_iota(jnp.int32, (TOK, BK), 1)
            ok = kpos >= start
            if causal:
                ok = ok & (kpos <= pos)
        for h in range(GQA):
            sl = pl.ds(h * TOK, TOK)
            s = lax.dot_general(q_s[sl, :], kb, (((1,), (1,)), ((), ())), preferred_element_type=F32)
            if masked or causal:
                s = jnp.where(ok, s, NEG)
            m_old = m_s[sl, :]
            m_new = jnp.maximum(m_old, jnp.max(s, axis=1, keepdims=True))
            p = jnp.exp2((s - m_new[:, :1]) * SCALE2)
            alpha = jnp.exp2((m_old - m_new) * SCALE2)
            m_s[sl, :] = m_new
            l_s[sl, :] = l_s[sl, :] * alpha + jnp.sum(p, axis=1, keepdims=True)
            acc_s[sl, :] = acc_s[sl, :] * alpha + jnp.dot(p.astype(BF), vb, preferred_element_type=F32)

    def loop(lo_, hi_, masked):
        def body_(j, carry):
            block(j, masked, False)
            return carry
        lax.fori_loop(lo_, hi_, body_, 0)

    loop(lo, full, True)
    loop(jnp.maximum(full, lo), diag, False)
    block(diag, True, True)
    for h in range(GQA):
        sl = pl.ds(h * TOK, TOK)
        out[:, h * 128:(h + 1) * 128] = (acc_s[sl, :] / l_s[sl, :]).astype(BF)


def attend(info, q_in, q_got, bias, cos, sin, ids, kv):
    vm = pl.BlockSpec(memory_space=pltpu.VMEM)
    hb = pl.BlockSpec(memory_space=pl.ANY)
    return pl.pallas_call(
        attend_kernel,
        out_shape=jax.ShapeDtypeStruct((TOK, GQA * HEAD_DIM), BF),
        in_specs=[pl.BlockSpec(memory_space=pltpu.SMEM)] + [vm] * 6 + [hb] * 20,
        out_specs=vm,
        scratch_shapes=[
            pltpu.VMEM((32 * TOK, HEAD_DIM), BF),
            pltpu.VMEM((32 * TOK, HEAD_DIM), BF),
            pltpu.VMEM((2, 32 * 16, HEAD_DIM), BF),
            pltpu.VMEM((GQA * TOK, HEAD_DIM), BF),
            pltpu.VMEM((GQA * TOK, HEAD_DIM), F32),
            pltpu.VMEM((GQA * TOK, HEAD_DIM), F32),
            pltpu.VMEM((GQA * TOK, HEAD_DIM), F32),
            pltpu.SemaphoreType.DMA((4,)),
        ],
        name="attend",
    )(info, q_in, q_got, bias, cos, sin, ids, *kv)


def kv_kernel(mine, got, bias, cos, sin, idrow, k_out, v_out):
    u = mine[...] + got[...] + bias[...].astype(F32)
    k_out[0:TOK, :] = rope(u[:, :HEAD_DIM], cos[...], sin[...]).astype(BF)
    v_out[0:TOK, :] = u[:, HEAD_DIM:].astype(BF)
    k_out[TOK:, :] = jnp.broadcast_to(idrow[0:1, :].astype(F32), (16, HEAD_DIM)).astype(BF)
    v_out[TOK:, :] = jnp.broadcast_to(idrow[1:2, :].astype(F32), (16, HEAD_DIM)).astype(BF)


def mix_kernel(blocks, a, w, o):
    o[...] = jnp.dot(a[...], w[...], preferred_element_type=F32).astype(o.dtype)


def mix(attended, out_weight, blocks, dtype):
    n = blocks.shape[0]
    return pl.pallas_call(
        mix_kernel,
        out_shape=jax.ShapeDtypeStruct((n, TOK, 1024), dtype),
        grid_spec=pltpu.PrefetchScalarGridSpec(
            num_scalar_prefetch=1,
            grid=(n,),
            in_specs=[
                pl.BlockSpec((TOK, 1024), lambda i, b: (0, 0)),
                pl.BlockSpec((1024, 1024), lambda i, b: (0, b[i])),
            ],
            out_specs=pl.BlockSpec((None, TOK, 1024), lambda i, b: (i, 0, 0)),
        ),
        name="mix",
    )(blocks, attended, out_weight)


def body(tokens, proj_weight, proj_bias, out_weight, doc_ids):
    x, y, z, c = (lax.axis_index(n) for n in ("grp", "y", "z", "c"))
    first = y * (8 * TOK) + z * (2 * TOK) + c * TOK
    quarter = lax.dynamic_slice(tokens.reshape(16, 4, 128, 256), (0, x, 0, 0), (16, 1, 128, 256)).reshape(16, 128, 256)
    got = lax.all_to_all(quarter, ("y", "z"), split_axis=0, concat_axis=0, tiled=True)
    wa, wb = plane_gather(proj_weight[:, :HALF], proj_weight[:, HALF:])
    got = got.reshape(4, 4, 128, 256)
    got = lax.dynamic_slice_in_dim(jnp.concatenate([got, got], axis=0), y, 4, axis=0)
    got = lax.dynamic_slice_in_dim(jnp.concatenate([got, got], axis=1), z, 4, axis=1)
    got = got.reshape(16, 128, 256)
    t_m, t_p = hop(got, "grp", 1), hop(got, "grp", -1)
    t_f = jnp.concatenate([hop(t_m[:8], "grp", 1), hop(t_p[8:], "grp", -1)], axis=0)
    ts = (got, t_p, t_f, t_m)
    offs = (0, 3, 1, 2)

    def halves(pieces, y_first):
        def src(o, other):
            return o * 4 + other if y_first else other * 4 + o
        near = [[src(o, d) for o in offs] for d in (0, 3, 1)]
        far = [[src(o, 2) for o in offs[:2]], [src(o, 2) for o in offs[2:]]]
        return project(ts, pieces[:3], near) + project(ts, pieces[3:], far)

    pa = halves(wa, True)
    pb = halves(wb, False)

    def rows(p, core):
        p = p.reshape(4, 128, p.shape[-1])
        return jnp.concatenate([
            lax.dynamic_index_in_dim(p, lax.rem(2 * core + j - x + 4, 4), 0, keepdims=False) for j in range(2)], axis=0)

    kv_part, q_part = pb[:, HALF - 256:], jnp.concatenate([pa, pb[:, :HALF - 256]], axis=1)
    kv_got = hop(rows(kv_part, 1 - c), "c", 1, 2)
    q_got = hop(rows(q_part, 1 - c), "c", 1, 2)
    bias = proj_bias.reshape(1, COLS)
    inverse_freq = theta_base ** (-(jnp.arange(HEAD_DIM // 2, dtype=F32) * 2.0) / HEAD_DIM)
    angles = (first + jnp.arange(TOK, dtype=jnp.int32)).astype(F32)[:, None] * inverse_freq[None, :]
    cos = jnp.concatenate([jnp.cos(angles), jnp.cos(angles)], axis=1)
    sin = jnp.concatenate([jnp.sin(angles), jnp.sin(angles)], axis=1)
    payload = jax.ShapeDtypeStruct((TOK + 16, HEAD_DIM), BF)
    k_own, v_own = pl.pallas_call(kv_kernel, out_shape=(payload, payload), name="kv")(
        rows(kv_part, c), kv_got, bias[:, 1024:], cos, sin, doc_ids.reshape(2, 128))
    k_all, v_all = plane_gather(k_own, v_own)
    mine = (*k_all, *v_all)
    other = tuple(hop(p, "c", 1, 2) for p in mine)
    info = jnp.stack([y, z, c]).astype(jnp.int32)
    attended = attend(info, rows(q_part, c), q_got, bias[:, :1024], cos, sin, doc_ids.reshape(TOK, 1), (*mine, *other))
    two = jnp.arange(2, dtype=jnp.int32)
    b_of = lambda d: lax.rem(x + d, 4).astype(jnp.int32) * 2 + two
    far = mix(attended, out_weight, b_of(2), BF)
    e_m, e_p = hop(far[0], "grp", 1), hop(far[1], "grp", -1)
    near = mix(attended, out_weight, jnp.concatenate([b_of(1), b_of(3), b_of(0)]), F32)
    to_p = jnp.concatenate([(near[0] + e_m.astype(F32)).astype(BF), near[1].astype(BF)], axis=1)
    to_m = jnp.concatenate([near[2].astype(BF), (near[3] + e_p.astype(F32)).astype(BF)], axis=1)
    r_m, r_p = hop(to_p, "grp", 1), hop(to_m, "grp", -1)
    own = jnp.concatenate([near[4], near[5]], axis=1)
    return (own + r_m.astype(F32) + r_p.astype(F32)).astype(BF)


def solution(mesh):
    fine = Mesh(mesh.devices.reshape(4, 4, 4, 2), ("grp", "y", "z", "c"))
    seq = ("y", "z", "c")
    return jax.shard_map(
        body,
        mesh=fine,
        in_specs=(P(None, seq), P(seq, "grp"), P("grp"), P("grp", None), P(seq)),
        out_specs=P(seq, "grp"),
        check_vma=False,
    )
```

```python
import functools
import jax
import jax.numpy as jnp
from jax import lax
from jax.experimental import pallas as pl
from jax.experimental.pallas import tpu as pltpu
from jax.sharding import Mesh, PartitionSpec as P


HEAD_DIM = 128
GQA = 8
TOK = 256
COLS = (GQA + 2) * HEAD_DIM
BK = 512
PAY = 2 * TOK + 16
OFFS = (0, 3, 1, 2)
theta_base = 1000000.0
NEG = -1e30
SCALE2 = HEAD_DIM ** -0.5 * 1.4426950408889634
BF = jnp.bfloat16
F32 = jnp.float32


def hop(x, axis, k, n=4):
    return lax.ppermute(x, axis, [(i, (i + k) % n) for i in range(n)])


def swap(x):
    return hop(x, "c", 1, 2)


def turn(x, k, second):
    pairs = []
    for y in range(4):
        for z in range(4):
            for c in range(2):
                along_y = (c == 0) != second
                to = ((y + k) % 4, z) if along_y else (y, (z + k) % 4)
                pairs.append((y * 8 + z * 2 + c, to[0] * 8 + to[1] * 2 + c))
    return lax.ppermute(x, ("y", "z", "c"), pairs)


def line_gather(x):
    return jnp.stack([x, turn(x, 1, False), turn(x, -1, False), turn(x, 2, False)])


def plane_gather(w):
    lo, hi = jnp.stack([w, turn(w, 1, False)]), jnp.stack([turn(w, -1, False), turn(w, 2, False)])
    lo, hi = lax.optimization_barrier((lo, hi))
    near = [turn(v, k, True) for k in (1, -1) for v in (lo, hi)]
    m_lo, m_hi, p_lo, p_hi = lax.optimization_barrier(tuple(near))
    f_lo, f_hi = turn(m_lo, 1, True), turn(p_hi, -1, True)
    return (lo, hi, m_lo, m_hi, p_lo, p_hi), (f_lo, f_hi)


def gather_rows(t, d):
    return jnp.concatenate([jnp.concatenate(
        [t[2 * k + n // 2][n % 2, d] for k in range(4)], axis=0) for n in range(4)], axis=1)


def token_specs(d):
    n, at = (4, 0) if d is None else (1, d)
    return [pl.BlockSpec((2, n, 128, 256), lambda i, *_: (0, at, 0, 0))] * 8


def near_kernel(*refs):
    t, ws, (out, lhs) = refs[:8], refs[8:14], refs[14:]

    @pl.when(pl.program_id(0) == 0)
    def _():
        for n, d in enumerate(OFFS[:3]):
            lhs[:, n * 1024:(n + 1) * 1024] = gather_rows(t, d)

    rhs = jnp.concatenate([w[...].reshape(512, 256) for w in ws], axis=0)
    out[...] = jnp.dot(lhs[...], rhs, preferred_element_type=F32)


def near_project(ts, ws):
    return pl.pallas_call(
        near_kernel,
        out_shape=jax.ShapeDtypeStruct((512, COLS), F32),
        grid=(5,),
        in_specs=token_specs(None) + [pl.BlockSpec((2, 256, 256), lambda i: (0, 0, i))] * 6,
        out_specs=pl.BlockSpec((512, 256), lambda i: (0, i)),
        scratch_shapes=[pltpu.VMEM((512, 3072), BF)],
        cost_estimate=pl.CostEstimate(flops=2 * 512 * 3072 * COLS, bytes_accessed=14 << 20, transcendentals=0),
        name="near",
    )(*ts, *ws)


def far_kernel(info, *refs, kv):
    t, (w0, w1, acc, mine, other, tot) = refs[:8], refs[8:]
    lhs = gather_rows(t, 0)
    rhs = jnp.concatenate([w0[...].reshape(512, 256), w1[...].reshape(512, 256)], axis=0)
    tot[...] = acc[...] + jnp.dot(lhs, rhs, preferred_element_type=F32)
    for b in range(4):
        k = lax.rem(b - info[0] + 4, 4)
        row = pl.ds(pl.multiple_of(k * 128, 128), 128)
        if kv:
            keys, values = tot[row, :128], tot[row, 128:]
            first = info[3] == 0
            mine[b * 128:(b + 1) * 128, :] = jnp.where(first, keys, values)
            other[b * 128:(b + 1) * 128, :] = jnp.where(first, values, keys)
        else:
            got = tot[row, :]
            at = slice((b % 2) * 128, (b % 2) * 128 + 128)

            @pl.when(info[3] == b // 2)
            def _(got=got, at=at):
                mine[at, :] = got

            @pl.when(info[3] != b // 2)
            def _(got=got, at=at):
                other[at, :] = got


def far_project(info, ts, ws, acc, kv):
    steps, base = (1, 4) if kv else (4, 0)
    half = jax.ShapeDtypeStruct((512, 128) if kv else (256, 1024), F32)
    ospec = pl.BlockSpec((512, 128) if kv else (256, 256), lambda i, _: (0, i))
    piece = pl.BlockSpec((2, 256, 256), lambda i, _: (0, 0, i + base))
    return pl.pallas_call(
        functools.partial(far_kernel, kv=kv),
        out_shape=(half, half),
        grid_spec=pltpu.PrefetchScalarGridSpec(
            num_scalar_prefetch=1,
            grid=(steps,),
            in_specs=token_specs(2) + [piece, piece, pl.BlockSpec((512, 256), lambda i, _: (0, i + base))],
            out_specs=(ospec, ospec),
            scratch_shapes=[pltpu.VMEM((512, 256), F32)],
        ),
        cost_estimate=pl.CostEstimate(flops=2 * 512 * 1024 * 256 * steps, bytes_accessed=5 << 20, transcendentals=0),
        name="far_kv" if kv else "far_q",
    )(info, *ts, *ws, acc)


def rope(u, cos, sin):
    turned = jnp.concatenate([-u[:, HEAD_DIM // 2:], u[:, :HEAD_DIM // 2]], axis=1)
    return u * cos + turned * sin


def attend_kernel(info, q_in, q_got, bias, cos, sin, ids, *refs):
    kv, (out, kv_s, q_s, m_s, l_s, acc_s, sems) = refs[:8], refs[8:]
    y, z, c = info[1], info[2], info[3]
    copies = []
    for side in range(2):
        kind = c if side == 0 else 1 - c
        for d, arr in zip(OFFS, kv[side * 4:side * 4 + 4]):
            for r, o in enumerate(OFFS):
                by = lax.rem(y + jnp.where(kind == 0, o, d), 4)
                bz = lax.rem(z + jnp.where(kind == 0, d, o), 4)
                copies.append(pltpu.make_async_copy(arr.at[r], kv_s.at[kind, by * 4 + bz], sems.at[side]))
    for cp in copies:
        cp.start()
    cs, sn = cos[...] * SCALE2, sin[...] * SCALE2
    for h in range(GQA):
        col = slice(h * 128, h * 128 + 128)
        u = q_in[:, col] + q_got[:, col] + bias[:, col].astype(F32)
        q_s[h] = rope(u, cs, sn).astype(BF)
    m_s[...] = jnp.full_like(m_s, NEG)
    l_s[...] = jnp.zeros_like(l_s)
    acc_s[...] = jnp.zeros_like(acc_s)
    for cp in copies:
        cp.wait()
    tail = kv_s[:, :, 512:528, :].astype(F32)
    used = lax.broadcasted_iota(jnp.int32, tail.shape, 2) < 2
    c1 = jnp.sum(jnp.where(used & (tail < 0.5), 1.0, 0.0)).astype(jnp.int32)
    c2 = jnp.sum(jnp.where(used & (tail < 1.5), 1.0, 0.0)).astype(jnp.int32)
    first = y * (8 * TOK) + z * (2 * TOK) + c * TOK
    last = first + TOK - 1
    start = jnp.where(ids[...] == 0, 0, jnp.where(ids[...] == 1, c1, c2))
    lo_start = jnp.where(first >= c2, c2, jnp.where(first >= c1, c1, 0))
    hi_start = jnp.where(last >= c2, c2, jnp.where(last >= c1, c1, 0))
    diag = first // BK
    lo = lo_start // BK
    full = jnp.clip((hi_start + BK - 1) // BK, lo, diag)
    pos = first + lax.broadcasted_iota(jnp.int32, (1, TOK), 1)

    def block(j, masked, causal):
        kb = kv_s[0, j, 0:BK, :]
        vt = jnp.concatenate([kv_s[1, j, 128 * n:128 * n + 128, :] for n in range(4)], axis=1)
        if masked or causal:
            kpos = j * BK + lax.broadcasted_iota(jnp.int32, (BK, TOK), 0)
            ok = kpos >= start
            if causal:
                ok = ok & (kpos <= pos)

        def score(h):
            s = lax.dot_general(kb, q_s[h], (((1,), (1,)), ((), ())), preferred_element_type=F32)
            return jnp.where(ok, s, NEG) if masked or causal else s

        s_next = score(0)
        for h in range(GQA):
            s = s_next
            if h + 1 < GQA:
                s_next = score(h + 1)
            m_old = m_s[h:h + 1, :]
            m_new = jnp.maximum(m_old, jnp.max(s, axis=0, keepdims=True))
            p = jnp.exp2(s - m_new)
            alpha = jnp.exp2(m_old - m_new)
            m_s[h:h + 1, :] = m_new
            l_s[h:h + 1, :] = l_s[h:h + 1, :] * alpha + jnp.sum(p, axis=0, keepdims=True)
            acc_s[h] = acc_s[h] * alpha + jnp.dot(vt, p.astype(BF), preferred_element_type=F32)

    def loop(lo_, hi_, masked):
        def body_(j, carry):
            block(j, masked, False)
            return carry

        lax.fori_loop(lo_, hi_, body_, 0)

    loop(lo, full, True)
    loop(full, diag, False)
    block(diag, True, True)
    for h in range(GQA):
        out[h] = jnp.transpose(acc_s[h] / l_s[h:h + 1, :]).astype(BF)


def attend(info, q_in, q_got, bias, cos, sin, ids, kv):
    vm = pl.BlockSpec(memory_space=pltpu.VMEM)
    hb = pl.BlockSpec(memory_space=pl.ANY)
    return pl.pallas_call(
        attend_kernel,
        out_shape=jax.ShapeDtypeStruct((GQA, TOK, HEAD_DIM), BF),
        in_specs=[pl.BlockSpec(memory_space=pltpu.SMEM)] + [vm] * 6 + [hb] * 8,
        out_specs=vm,
        scratch_shapes=[
            pltpu.VMEM((2, 16, PAY, HEAD_DIM), BF),
            pltpu.VMEM((GQA, TOK, HEAD_DIM), BF),
            pltpu.VMEM((GQA, TOK), F32),
            pltpu.VMEM((GQA, TOK), F32),
            pltpu.VMEM((GQA, HEAD_DIM, TOK), F32),
            pltpu.SemaphoreType.DMA((2,)),
        ],
        cost_estimate=pl.CostEstimate(flops=10 ** 10, bytes_accessed=6 << 20, transcendentals=10 ** 7),
        name="attend",
    )(info, q_in, q_got, bias, cos, sin, ids, *kv)


def kv_kernel(info, mine, got, bias, cos, sin, idrow, out):
    u = mine[...] + got[...]

    @pl.when(info[3] == 0)
    def _():
        out[0:512, :] = rope(u + bias[:, :HEAD_DIM].astype(F32), cos[...], sin[...]).astype(BF)

    @pl.when(info[3] == 1)
    def _():
        v = u + bias[:, HEAD_DIM:].astype(F32)
        for n in range(4):
            out[n * 128:(n + 1) * 128, :] = jnp.transpose(v[n * 128:(n + 1) * 128, :]).astype(BF)

    sel = lax.broadcasted_iota(jnp.int32, (16, HEAD_DIM), 0) == 0
    r0 = jnp.broadcast_to(idrow[0:1, :], (16, HEAD_DIM)).astype(F32)
    r1 = jnp.broadcast_to(idrow[1:2, :], (16, HEAD_DIM)).astype(F32)
    out[512:528, :] = jnp.where(sel, r0, r1).astype(BF)


def mix_kernel(info, *refs, plan, last):
    atts, refs = refs[:len(plan) + last], refs[len(plan) + last:]
    acc, refs = (refs[0], refs[1:]) if last else (None, refs)
    ds = sorted({d for _, use in plan for d in use})
    w, (out, w0, w1, tot, att, sems) = refs[:4 * len(ds)], refs[4 * len(ds):]
    x, y, z, c = (info[i] for i in range(4))
    terms = [(i, k, d) for i, (k, use) in enumerate(plan) for d in use]
    by_d = [[t for t in terms if t[2] == d] for d in ds]
    spot1 = {t: sum(len(g) for g in by_d[:m]) + g.index(t) for m, g in enumerate(by_d) for t in g}
    for side in range(2):
        for is_one in range(2):
            @pl.when((c if side == 0 else 1 - c) == is_one)
            def _(side=side, is_one=is_one):
                for at, t in enumerate(terms):
                    for n in range(4):
                        src = w[(side * len(ds) + ds.index(t[2])) * 2 + n // 2].at[n % 2, lax.rem(x + t[1], 4)]
                        dst = w1.at[pl.ds((spot1[t] * 4 + n) * 128, 128)] if is_one else w0.at[n, pl.ds(at * 128, 128)]
                        pltpu.make_async_copy(src, dst, sems.at[is_one]).start()
    for i, (k, _) in enumerate(plan):
        if k == 2:
            for m in range(2):
                att[i, m * 4:m * 4 + 4] = atts[i + m][...]
        else:
            att[i] = atts[i][...]
    for cc in range(4):
        col = slice(cc * 512, cc * 512 + 512)
        tot[cc] = acc[:, col] if last else jnp.zeros((TOK, 512), F32)
    pltpu.make_async_copy(w0, w0, sems.at[0]).wait()
    lhs = jnp.concatenate([att[i, lax.rem(z + d, 4) * 2] for i, k, d in terms], axis=1)
    for n in range(4):
        tot[lax.rem(y + OFFS[n], 4)] += jnp.dot(lhs, w0[n], preferred_element_type=F32)
    pltpu.make_async_copy(w1, w1, sems.at[1]).wait()
    row = 0
    for d, g in zip(ds, by_d):
        lhs = jnp.concatenate([att[i, lax.rem(z + o, 4) * 2 + 1] for i, k, _ in g for o in OFFS], axis=1)
        tot[lax.rem(y + d, 4)] += jnp.dot(lhs, w1[row:row + 512 * len(g), :], preferred_element_type=F32)
        row += 512 * len(g)
    for cc in range(4):
        out[:, cc * 512:cc * 512 + 512] = tot[cc].astype(out.dtype)


def mix(info, atts, acc, w, plan):
    vm = pl.BlockSpec(memory_space=pltpu.VMEM)
    last = acc is not None
    args = (info, *atts, *((acc,) if last else ()))
    work = sum(len(use) for _, use in plan)
    return pl.pallas_call(
        functools.partial(mix_kernel, plan=plan, last=last),
        out_shape=jax.ShapeDtypeStruct((TOK, 2048), BF if last else F32),
        in_specs=[pl.BlockSpec(memory_space=pltpu.SMEM)] + [vm] * (len(args) - 1) + [pl.BlockSpec(memory_space=pl.ANY)] * len(w),
        out_specs=vm,
        scratch_shapes=[
            pltpu.VMEM((4, work * 128, 512), BF), pltpu.VMEM((work * 512, 512), BF), pltpu.VMEM((4, TOK, 512), F32),
            pltpu.VMEM((len(plan), GQA, TOK, 128), BF), pltpu.SemaphoreType.DMA((2,))],
        cost_estimate=pl.CostEstimate(flops=work * 2 ** 28, bytes_accessed=work << 20, transcendentals=0),
        name="mix",
    )(*args, *w)


def layer(tokens, proj_weight, proj_bias, out_weight, doc_ids):
    x, y, z, c = (lax.axis_index(n) for n in ("grp", "y", "z", "c"))
    quarter = lax.dynamic_slice(tokens.reshape(16, 4, 128, 256), (0, x, 0, 0), (16, 1, 128, 256)).reshape(16, 128, 256)
    got = lax.all_to_all(quarter, ("y", "z"), split_axis=0, concat_axis=0, tiled=True)
    near_w, far_w = plane_gather(proj_weight)
    rows = lax.dynamic_slice_in_dim(out_weight, (2 * z + c) * 128, 128, axis=0)
    share = jnp.stack([lax.dynamic_slice_in_dim(rows, n * 2048 + y * 512, 512, axis=1) for n in range(4)])
    share = lax.all_to_all(share, "grp", split_axis=0, concat_axis=0, tiled=True)
    near_o, far_o = plane_gather(share)
    got = got.reshape(4, 4, 128, 256)
    got = lax.dynamic_slice_in_dim(jnp.concatenate([got, got], axis=0), y, 4, axis=0)
    got = lax.dynamic_slice_in_dim(jnp.concatenate([got, got], axis=1), z, 4, axis=1)
    got = jnp.where(c == 0, got, jnp.transpose(got, (1, 0, 2, 3)))
    g = jnp.stack([got[0], got[3]]), jnp.stack([got[1], got[2]])
    t_m, t_p = [hop(v, "grp", 1) for v in g], [hop(v, "grp", -1) for v in g]
    t_f = hop(t_m[0], "grp", 1), hop(t_p[1], "grp", -1)
    ts = (*g, *t_p, *t_f, *t_m)
    info = jnp.stack([x, y, z, c]).astype(jnp.int32)
    acc = near_project(ts, near_w)
    kv_mine, kv_other = far_project(info, ts, far_w, acc, True)
    kv_got = swap(kv_other)
    q_mine, q_other = far_project(info, ts, far_w, acc, False)
    q_got = swap(q_other)
    bias = proj_bias.reshape(1, COLS)
    inverse_freq = theta_base ** (-(jnp.arange(HEAD_DIM // 2, dtype=F32) * 2.0) / HEAD_DIM)
    chip = y * (8 * TOK) + z * (2 * TOK)
    angles = (chip + jnp.arange(2 * TOK, dtype=jnp.int32)).astype(F32)[:, None] * inverse_freq[None, :]
    cos = jnp.concatenate([jnp.cos(angles), jnp.cos(angles)], axis=1)
    sin = jnp.concatenate([jnp.sin(angles), jnp.sin(angles)], axis=1)
    cos_q, sin_q = (lax.dynamic_slice_in_dim(t, c * TOK, TOK, axis=0) for t in (cos, sin))
    vm = pl.BlockSpec(memory_space=pltpu.VMEM)
    payload = pl.pallas_call(
        kv_kernel, out_shape=jax.ShapeDtypeStruct((PAY, HEAD_DIM), BF), name="kv",
        in_specs=[pl.BlockSpec(memory_space=pltpu.SMEM)] + [vm] * 6, out_specs=vm)(
        info, kv_mine, kv_got, bias[:, 1024:], cos, sin, doc_ids.reshape(2, 128))
    line = line_gather(payload)
    km, kp, kf = turn(line, 1, True), turn(line, -1, True), turn(line, 2, True)
    mine = (line, km, kp, kf)
    other = (swap(line),)
    other += tuple(swap(p) for p in mine[1:])
    attended = attend(info, q_mine, q_got, bias[:, :1024], cos_q, sin_q, doc_ids.reshape(1, TOK), mine + other)
    w_near = near_o[:2] + near_o[4:] + near_o[2:4]
    near_w2 = w_near + tuple(swap(p) for p in w_near)
    far_pair = far_o + tuple(swap(p) for p in far_o)
    a_m, a_p = hop(attended, "grp", 1), hop(attended, "grp", -1)
    a_f = hop(a_m[:4], "grp", 1), hop(a_p[4:], "grp", -1)
    atts = (attended, a_p, a_m)
    acc = mix(info, atts, None, near_w2, ((0, (0, 1, 3)), (1, (0, 1, 3)), (3, (0, 1, 3))))
    w_all = near_w2[:4] + far_pair[:2] + near_w2[4:6] + near_w2[6:10] + far_pair[2:] + near_w2[10:]
    return mix(info, atts + a_f, acc, w_all, ((0, (2,)), (1, (2,)), (3, (2,)), (2, (0, 1, 2, 3))))


def solution(mesh):
    fine = Mesh(mesh.devices.reshape(4, 4, 4, 2), ("grp", "y", "z", "c"))
    seq = ("y", "z", "c")
    return jax.shard_map(
        layer,
        mesh=fine,
        in_specs=(P(None, seq), P(seq, "grp"), P("grp"), P("grp", None), P(seq)),
        out_specs=P(seq, "grp"),
        check_vma=False,
    )
```

```python
import functools
import jax
import jax.numpy as jnp
from jax import lax
from jax.experimental import pallas as pl
from jax.experimental.pallas import tpu as pltpu
from jax.sharding import Mesh, PartitionSpec as P


HEAD_DIM = 128
GQA = 8
TOK = 256
COLS = (GQA + 2) * HEAD_DIM
BK = 512
PAY = 2 * TOK + 16
OFFS = (0, 3, 1, 2)
theta_base = 1000000.0
NEG = -1e30
SCALE2 = HEAD_DIM ** -0.5 * 1.4426950408889634
BF = jnp.bfloat16
F32 = jnp.float32


def hop(x, axis, k, n=4):
    return lax.ppermute(x, axis, [(i, (i + k) % n) for i in range(n)])


def swap(x):
    return hop(x, "c", 1, 2)


def turn(x, k, second):
    pairs = []
    for y in range(4):
        for z in range(4):
            for c in range(2):
                along_y = (c == 0) != second
                to = ((y + k) % 4, z) if along_y else (y, (z + k) % 4)
                pairs.append((y * 8 + z * 2 + c, to[0] * 8 + to[1] * 2 + c))
    return lax.ppermute(x, ("y", "z", "c"), pairs)


def line_gather(x):
    return jnp.stack([x, turn(x, 1, False), turn(x, -1, False), turn(x, 2, False)])


def plane_gather(w):
    lo, hi = jnp.stack([w, turn(w, 1, False)]), jnp.stack([turn(w, -1, False), turn(w, 2, False)])
    lo, hi = lax.optimization_barrier((lo, hi))
    near = [turn(v, k, True) for k in (1, -1) for v in (lo, hi)]
    m_lo, m_hi, p_lo, p_hi = lax.optimization_barrier(tuple(near))
    f_lo, f_hi = turn(m_lo, 1, True), turn(p_hi, -1, True)
    return (lo, hi, m_lo, m_hi, p_lo, p_hi), (f_lo, f_hi)


def gather_rows(pairs, d):
    return jnp.concatenate([jnp.concatenate(
        [p[n // 2][n % 2, d] for p in pairs], axis=0) for n in range(4)], axis=1)


def near_kernel(*refs):
    t, ws, (out, lhs) = refs[:6], refs[6:12], refs[12:]

    @pl.when(pl.program_id(0) == 0)
    def _():
        for n, d in enumerate(OFFS[:3]):
            lhs[:, n * 1024:(n + 1) * 1024] = gather_rows((t[:2], t[2:4], t[4:]), d)

    rhs = jnp.concatenate([w[...].reshape(512, 256) for w in ws], axis=0)
    out[...] = jnp.dot(lhs[...], rhs, preferred_element_type=F32)


def near_project(ts, ws):
    return pl.pallas_call(
        near_kernel,
        out_shape=jax.ShapeDtypeStruct((384, COLS), F32),
        grid=(5,),
        in_specs=[pl.BlockSpec((2, 4, 128, 256), lambda i: (0, 0, 0, 0))] * 6
        + [pl.BlockSpec((2, 256, 256), lambda i: (0, 0, i))] * 6,
        out_specs=pl.BlockSpec((384, 256), lambda i: (0, i)),
        scratch_shapes=[pltpu.VMEM((384, 3072), BF)],
        cost_estimate=pl.CostEstimate(flops=2 * 384 * 3072 * COLS, bytes_accessed=14 << 20, transcendentals=0),
        name="near",
    )(*ts, *ws)


def far_kernel(info, *refs, kv):
    t, f, ws, (acc, mine, other, tot) = refs[:6], refs[6:8], refs[8:16], refs[16:]
    rhs = [w[...].reshape(512, 256) for w in ws]
    part = jnp.dot(
        gather_rows((t[:2], t[2:4], t[4:]), 0), jnp.concatenate(rhs[6:], axis=0), preferred_element_type=F32)
    new = jnp.dot(
        jnp.concatenate([gather_rows((f,), d) for d in OFFS], axis=1), jnp.concatenate(rhs, axis=0),
        preferred_element_type=F32)
    tot[0:256, :] = acc[0:256, :] + part[0:256, :]
    tot[256:384, :] = new
    tot[384:512, :] = acc[256:384, :] + part[256:384, :]
    for b in range(4):
        k = lax.rem(b - info[0] + 4, 4)
        row = pl.ds(pl.multiple_of(k * 128, 128), 128)
        if kv:
            keys, values = tot[row, :128], tot[row, 128:]
            first = info[3] == 0
            mine[b * 128:(b + 1) * 128, :] = jnp.where(first, keys, values)
            other[b * 128:(b + 1) * 128, :] = jnp.where(first, values, keys)
        else:
            got = tot[row, :]
            at = slice((b % 2) * 128, (b % 2) * 128 + 128)

            @pl.when(info[3] == b // 2)
            def _(got=got, at=at):
                mine[at, :] = got

            @pl.when(info[3] != b // 2)
            def _(got=got, at=at):
                other[at, :] = got


def far_project(info, ts, fs, ws, acc, kv):
    steps, base = (1, 4) if kv else (4, 0)
    half = jax.ShapeDtypeStruct((512, 128) if kv else (256, 1024), F32)
    ospec = pl.BlockSpec((512, 128) if kv else (256, 256), lambda i, _: (0, i))
    return pl.pallas_call(
        functools.partial(far_kernel, kv=kv),
        out_shape=(half, half),
        grid_spec=pltpu.PrefetchScalarGridSpec(
            num_scalar_prefetch=1,
            grid=(steps,),
            in_specs=[pl.BlockSpec((2, 1, 128, 256), lambda i, _: (0, 2, 0, 0))] * 6
            + [pl.BlockSpec((2, 4, 128, 256), lambda i, _: (0, 0, 0, 0))] * 2
            + [pl.BlockSpec((2, 256, 256), lambda i, _: (0, 0, i + base))] * 8
            + [pl.BlockSpec((384, 256), lambda i, _: (0, i + base))],
            out_specs=(ospec, ospec),
            scratch_shapes=[pltpu.VMEM((512, 256), F32)],
        ),
        cost_estimate=pl.CostEstimate(flops=2 * 512 * 2048 * 256 * steps, bytes_accessed=5 << 20, transcendentals=0),
        name="far_kv" if kv else "far_q",
    )(info, *ts, *fs, *ws, acc)


def rope(u, cos, sin):
    turned = jnp.concatenate([-u[:, HEAD_DIM // 2:], u[:, :HEAD_DIM // 2]], axis=1)
    return u * cos + turned * sin


def attend_kernel(info, q_in, q_got, bias, cos, sin, ids, *refs):
    kv, (lo_out, hi_out, kv_s, q_s, m_s, l_s, acc_s, sems) = refs[:8], refs[8:]
    y, z, c = info[1], info[2], info[3]
    copies = []
    for side in range(2):
        kind = c if side == 0 else 1 - c
        for d, arr in zip(OFFS, kv[side * 4:side * 4 + 4]):
            for r, o in enumerate(OFFS):
                by = lax.rem(y + jnp.where(kind == 0, o, d), 4)
                bz = lax.rem(z + jnp.where(kind == 0, d, o), 4)
                copies.append(pltpu.make_async_copy(arr.at[r], kv_s.at[kind, by * 4 + bz], sems.at[side]))
    for cp in copies:
        cp.start()
    own = pl.ds(pl.multiple_of(c * TOK, TOK), TOK)
    cs, sn = cos[own, :] * SCALE2, sin[own, :] * SCALE2
    for h in range(GQA):
        col = slice(h * 128, h * 128 + 128)
        u = q_in[:, col] + q_got[:, col] + bias[:, col].astype(F32)
        q_s[h] = rope(u, cs, sn).astype(BF)
    m_s[...] = jnp.full_like(m_s, NEG)
    l_s[...] = jnp.zeros_like(l_s)
    acc_s[...] = jnp.zeros_like(acc_s)
    for cp in copies:
        cp.wait()
    tail = kv_s[:, :, 512:528, :].astype(F32)
    used = lax.broadcasted_iota(jnp.int32, tail.shape, 2) < 2
    c1 = jnp.sum(jnp.where(used & (tail < 0.5), 1.0, 0.0)).astype(jnp.int32)
    c2 = jnp.sum(jnp.where(used & (tail < 1.5), 1.0, 0.0)).astype(jnp.int32)
    first = y * (8 * TOK) + z * (2 * TOK) + c * TOK
    last = first + TOK - 1
    start = jnp.where(ids[...] == 0, 0, jnp.where(ids[...] == 1, c1, c2))
    lo_start = jnp.where(first >= c2, c2, jnp.where(first >= c1, c1, 0))
    hi_start = jnp.where(last >= c2, c2, jnp.where(last >= c1, c1, 0))
    diag = first // BK
    lo = lo_start // BK
    full = jnp.clip((hi_start + BK - 1) // BK, lo, diag)
    pos = first + lax.broadcasted_iota(jnp.int32, (1, TOK), 1)

    def block(j, masked, causal):
        kb = kv_s[0, j, 0:BK, :]
        vt = jnp.concatenate([kv_s[1, j, 128 * n:128 * n + 128, :] for n in range(4)], axis=1)
        if masked or causal:
            kpos = j * BK + lax.broadcasted_iota(jnp.int32, (BK, TOK), 0)
            ok = kpos >= start
            if causal:
                ok = ok & (kpos <= pos)

        def score(h):
            s = lax.dot_general(kb, q_s[h], (((1,), (1,)), ((), ())), preferred_element_type=F32)
            return jnp.where(ok, s, NEG) if masked or causal else s

        ss = [score(h) for h in range(2)]
        queue = []
        for h in range(GQA + 1):
            if h < GQA:
                s = ss.pop(0)
                if h + 2 < GQA:
                    ss.append(score(h + 2))
                m_old = m_s[h:h + 1, :]
                m_new = jnp.maximum(m_old, jnp.max(s, axis=0, keepdims=True))
                p = jnp.exp2(s - m_new)
                alpha = jnp.exp2(m_old - m_new)
                m_s[h:h + 1, :] = m_new
                l_s[h:h + 1, :] = l_s[h:h + 1, :] * alpha + jnp.sum(p, axis=0, keepdims=True)
                queue.append((h, p.astype(BF), alpha))
            if h >= 1:
                held = queue.pop(0)
                g = held[0]
                r = jnp.dot(vt, held[1], preferred_element_type=F32)
                acc_s[g] = acc_s[g] * held[2] + r

    def loop(lo_, hi_, masked):
        def body_(j, carry):
            block(j, masked, False)
            return carry

        lax.fori_loop(lo_, hi_, body_, 0)

    loop(lo, full, True)
    loop(full, diag, False)
    block(diag, True, True)
    for h in range(GQA):
        (lo_out, hi_out)[h // 4][h % 4] = jnp.transpose(acc_s[h] / l_s[h:h + 1, :]).astype(BF)


def attend(info, q_in, q_got, bias, cos, sin, ids, kv):
    vm = pl.BlockSpec(memory_space=pltpu.VMEM)
    hb = pl.BlockSpec(memory_space=pl.ANY)
    return pl.pallas_call(
        attend_kernel,
        out_shape=(jax.ShapeDtypeStruct((GQA // 2, TOK, HEAD_DIM), BF),) * 2,
        in_specs=[pl.BlockSpec(memory_space=pltpu.SMEM)] + [vm] * 6 + [hb] * 8,
        out_specs=(vm, vm),
        scratch_shapes=[
            pltpu.VMEM((2, 16, PAY, HEAD_DIM), BF),
            pltpu.VMEM((GQA, TOK, HEAD_DIM), BF),
            pltpu.VMEM((GQA, TOK), F32),
            pltpu.VMEM((GQA, TOK), F32),
            pltpu.VMEM((GQA, HEAD_DIM, TOK), F32),
            pltpu.SemaphoreType.DMA((2,)),
        ],
        cost_estimate=pl.CostEstimate(flops=10 ** 10, bytes_accessed=6 << 20, transcendentals=10 ** 7),
        name="attend",
    )(info, q_in, q_got, bias, cos, sin, ids, *kv)


def kv_kernel(info, mine, got, bias, cos, sin, idrow, out):
    u = mine[...] + got[...]

    @pl.when(info[3] == 0)
    def _():
        out[0:512, :] = rope(u + bias[:, COLS - 256:COLS - 128].astype(F32), cos[...], sin[...]).astype(BF)

    @pl.when(info[3] == 1)
    def _():
        v = u + bias[:, COLS - 128:].astype(F32)
        for n in range(4):
            out[n * 128:(n + 1) * 128, :] = jnp.transpose(v[n * 128:(n + 1) * 128, :]).astype(BF)

    sel = lax.broadcasted_iota(jnp.int32, (16, HEAD_DIM), 0) == 0
    r0 = jnp.broadcast_to(idrow[0:1, :], (16, HEAD_DIM)).astype(F32)
    r1 = jnp.broadcast_to(idrow[1:2, :], (16, HEAD_DIM)).astype(F32)
    out[512:528, :] = jnp.where(sel, r0, r1).astype(BF)


def mix_kernel(info, *refs, plan, last):
    atts, refs = refs[:2 * len(plan)], refs[2 * len(plan):]
    acc, refs = (refs[0], refs[1:]) if last else (None, refs)
    ds = sorted({d for _, use in plan for d in use})
    w, (out, w0, w1, tot, att, sems) = refs[:4 * len(ds)], refs[4 * len(ds):]
    early = [pltpu.make_async_copy(v, att.at[n // 2, pl.ds((n % 2) * 4, 4)], sems.at[2]) for n, v in enumerate(atts)]
    early += [pltpu.make_async_copy(acc.at[:, pl.ds(cc * 512, 512)], tot.at[cc], sems.at[3]) for cc in range(4)] if last else []
    for cp in early:
        cp.start()
    _, y, z, c = (info[i] for i in range(4))
    terms = [(i, k, d) for i, (k, use) in enumerate(plan) for d in use]
    by_d = [[t for t in terms if t[2] == d] for d in ds]
    spot1 = {t: sum(len(g) for g in by_d[:m]) + g.index(t) for m, g in enumerate(by_d) for t in g}
    for side in range(2):
        for is_one in range(2):
            @pl.when((c if side == 0 else 1 - c) == is_one)
            def _(side=side, is_one=is_one):
                for at, t in enumerate(terms):
                    for n in range(4):
                        src = w[(side * len(ds) + ds.index(t[2])) * 2 + n // 2].at[n % 2, (4 - t[1]) % 4]
                        dst = w1.at[pl.ds((spot1[t] * 4 + n) * 128, 128)] if is_one else w0.at[n, pl.ds(at * 128, 128)]
                        pltpu.make_async_copy(src, dst, sems.at[is_one]).start()
    if last:
        pltpu.make_async_copy(tot, tot, sems.at[3]).wait()
    else:
        tot[...] = jnp.zeros_like(tot)
    pltpu.make_async_copy(att, att, sems.at[2]).wait()
    pltpu.make_async_copy(w0, w0, sems.at[0]).wait()
    lhs = jnp.concatenate([att[i, lax.rem(z + d, 4) * 2] for i, k, d in terms], axis=1)
    for n in range(4):
        tot[lax.rem(y + OFFS[n], 4)] += jnp.dot(lhs, w0[n], preferred_element_type=F32)
    pltpu.make_async_copy(w1, w1, sems.at[1]).wait()
    row = 0
    for d, g in zip(ds, by_d):
        lhs = jnp.concatenate([att[i, lax.rem(z + o, 4) * 2 + 1] for i, k, _ in g for o in OFFS], axis=1)
        tot[lax.rem(y + d, 4)] += jnp.dot(lhs, w1[row:row + 512 * len(g), :], preferred_element_type=F32)
        row += 512 * len(g)
    for cc in range(4):
        out[:, cc * 512:cc * 512 + 512] = tot[cc].astype(out.dtype)


def mix(info, atts, acc, w, plan):
    vm = pl.BlockSpec(memory_space=pltpu.VMEM)
    last = acc is not None
    args = (info, *atts, *((acc,) if last else ()))
    work = sum(len(use) for _, use in plan)
    return pl.pallas_call(
        functools.partial(mix_kernel, plan=plan, last=last),
        out_shape=jax.ShapeDtypeStruct((TOK, 2048), BF if last else F32),
        in_specs=[pl.BlockSpec(memory_space=pltpu.SMEM)] + [pl.BlockSpec(memory_space=pl.ANY)] * (len(args) - 1 + len(w)),
        out_specs=vm,
        scratch_shapes=[
            pltpu.VMEM((4, work * 128, 512), BF), pltpu.VMEM((work * 512, 512), BF), pltpu.VMEM((4, TOK, 512), F32),
            pltpu.VMEM((len(plan), GQA, TOK, 128), BF), pltpu.SemaphoreType.DMA((4,))],
        cost_estimate=pl.CostEstimate(flops=work * 2 ** 28, bytes_accessed=work << 20, transcendentals=0),
        name="mix_far" if last else "mix_near",
    )(*args, *w)


def layer(tokens, proj_weight, proj_bias, out_weight, doc_ids):
    x, y, z, c = (lax.axis_index(n) for n in ("grp", "y", "z", "c"))
    quarter = lax.dynamic_slice(tokens.reshape(16, 4, 128, 256), (0, x, 0, 0), (16, 1, 128, 256)).reshape(16, 128, 256)
    got = lax.all_to_all(quarter, ("y", "z"), split_axis=0, concat_axis=0, tiled=True)
    near_w, far_w = plane_gather(proj_weight)
    rows = lax.dynamic_slice_in_dim(out_weight, (2 * z + c) * 128, 128, axis=0)
    part = lambda k: lax.dynamic_slice_in_dim(rows, lax.rem(x + k, 4) * 2048 + y * 512, 512, axis=1)
    share = [part(0)] + [hop(part(k), "grp", k) for k in (1, 2, 3)]
    share = jnp.stack(share)
    near_o, far_o = plane_gather(share)
    got = got.reshape(4, 4, 128, 256)
    got = lax.dynamic_slice_in_dim(jnp.concatenate([got, got], axis=0), y, 4, axis=0)
    got = lax.dynamic_slice_in_dim(jnp.concatenate([got, got], axis=1), z, 4, axis=1)
    got = jnp.where(c == 0, got, jnp.transpose(got, (1, 0, 2, 3)))
    g = jnp.stack([got[0], got[3]]), jnp.stack([got[1], got[2]])
    t_m, t_p = [hop(v, "grp", 1) for v in g], [hop(v, "grp", -1) for v in g]
    t_f = hop(t_m[0], "grp", 1), hop(t_p[1], "grp", -1)
    ts = (*g, *t_p, *t_m)
    info = jnp.stack([x, y, z, c]).astype(jnp.int32)
    acc = near_project(ts, near_w)
    kv_mine, kv_other = far_project(info, ts, t_f, near_w + far_w, acc, True)
    kv_got = swap(kv_other)
    q_mine, q_other = far_project(info, ts, t_f, near_w + far_w, acc, False)
    q_got = swap(q_other)
    bias = proj_bias.reshape(1, COLS)
    inverse_freq = theta_base ** (-(jnp.arange(HEAD_DIM // 2, dtype=F32) * 2.0) / HEAD_DIM)
    chip = y * (8 * TOK) + z * (2 * TOK)
    angles = (chip + jnp.arange(2 * TOK, dtype=jnp.int32)).astype(F32)[:, None] * inverse_freq[None, :]
    cos = jnp.concatenate([jnp.cos(angles), jnp.cos(angles)], axis=1)
    sin = jnp.concatenate([jnp.sin(angles), jnp.sin(angles)], axis=1)
    vm = pl.BlockSpec(memory_space=pltpu.VMEM)
    payload = pl.pallas_call(
        kv_kernel, out_shape=jax.ShapeDtypeStruct((PAY, HEAD_DIM), BF), name="kv",
        in_specs=[pl.BlockSpec(memory_space=pltpu.SMEM)] + [vm] * 6, out_specs=vm)(
        info, kv_mine, kv_got, bias, cos, sin, doc_ids.reshape(2, 128))
    line = line_gather(payload)
    km, kp, kf = turn(line, 1, True), turn(line, -1, True), turn(line, 2, True)
    mine = (line, km, kp, kf)
    other = (swap(line),)
    other += tuple(swap(p) for p in mine[1:])
    attended = attend(info, q_mine, q_got, bias, cos, sin, doc_ids.reshape(1, TOK), mine + other)
    w_near = near_o[:2] + near_o[4:] + near_o[2:4]
    near_w2 = w_near + tuple(swap(p) for p in w_near)
    far_pair = far_o + tuple(swap(p) for p in far_o)
    a_m, a_p = [hop(v, "grp", 1) for v in attended], [hop(v, "grp", -1) for v in attended]
    a_f = [hop(a_m[0], "grp", 1), hop(a_p[1], "grp", -1)]
    atts = (*attended, *a_p, *a_m)
    acc = mix(info, atts, None, near_w2, ((0, (0, 1, 3)), (1, (0, 1, 3)), (3, (0, 1, 3))))
    w_all = near_w2[:4] + far_pair[:2] + near_w2[4:6] + near_w2[6:10] + far_pair[2:] + near_w2[10:]
    return mix(info, (*atts, *a_f), acc, w_all, ((0, (2,)), (1, (2,)), (3, (2,)), (2, (0, 1, 2, 3))))


def solution(mesh):
    fine = Mesh(mesh.devices.reshape(4, 4, 4, 2), ("grp", "y", "z", "c"))
    seq = ("y", "z", "c")
    return jax.shard_map(
        layer,
        mesh=fine,
        in_specs=(P(None, seq), P(seq, "grp"), P("grp"), P("grp", None), P(seq)),
        out_specs=P(seq, "grp"),
        check_vma=False,
    )
```
